512 devices in a mesh: groups: 2 (over y), batch: 128 (over z, x), mp: 2 (over core).
Axes of the slice: x: 4, y: 2, z: 32, core: 2. Of those that a mesh axis runs over, the one named last changes fastest.
The devices are a block of a 4x8x32 slice.
Arguments:
- hidden: bfloat16 [512, 1280], P(('groups', 'batch')), parts along dimension 0, may hold values from -6 to 6
- token_qkv: bfloat16 [3, 512, 1280], P(None, ('groups', 'batch'), 'mp'), parts along dimension 1, may hold values from -6 to 6
- self_cache: bfloat16 [2, 512, 128, 1280], P(None, ('groups', 'batch'), None, 'mp'), parts along dimension 1, may hold values from -6 to 6
- cross_kv: bfloat16 [2, 512, 64, 1280], P(None, ('groups', 'batch'), None, 'mp'), parts along dimension 1, may hold values from -6 to 6
- cache_len: int32 [512], P(('groups', 'batch')), parts along dimension 0, may hold values from 1 to 127
- finished: int32 [512], P(('groups', 'batch')), parts along dimension 0, may hold values 0 or 1
- new_slot: int32 [512], P(('groups', 'batch')), parts along dimension 0, may hold values from 0 to 255, as said below
- out_proj: bfloat16 [1280, 1280], P('mp'), may hold values from -0.15625 to 0.15625
- ln_gain: float32 [1280], replicated, may hold values from 0.5 to 1.5
- ln_bias: float32 [1280], replicated, may hold values from -3 to 3
- query_proj: bfloat16 [1280, 1280], P(None, 'mp'), may hold values from -3 to 3
Outputs:
- moved_cache: bfloat16 [2, 512, 128, 1280], P(None, ('groups', 'batch'), None, 'mp'), parts along dimension 1
- moved_out: bfloat16 [512, 1280], P(('groups', 'batch'), 'mp'), parts along dimension 0
The draws below stay inside these ranges and needn't reach their ends.
There are 2 independent parts, one for each index of `groups`. The reference program is written for one: setup_inputs(seed, part) draws one part's arguments, and reference() takes and returns one part's arrays. A program takes and returns all parts, laid end to end along the dimension named above; an argument that names none is the same for every part. Nothing has to cross between parts.
Inputs may be any that keep to these rules, and one draw needn't show every extreme that they name: A permutation of the spans' slots. Span c's new owner new_slot[c] // 2 lies within 3 devices of its present one c // 2, counting the device order as a loop; of one device's spans at most one moves by any given signed distance.
All inputs are finite; a program needn't handle non-finite values. No bound on the sum of `finished` on one device may be relied on, other than what follows from the above.
Results may differ from the reference program's by a relative error of at most 0.015.
Values may be sent and summed in bfloat16 or wider, within the bound.
A program may use at most 64 MiB of HBM per device.

```python
import jax
import jax.numpy as jnp
from jax import lax

D = 1280
HEADS = 20
HEAD_DIM = 64
CH_DEV = 2
ENC = 64
SLOTS = 128
SPANS = 256


def swap_round(key, table, stride, period):
    devices, width = table.shape
    keys = jax.random.split(key, 4)
    phase = jax.random.randint(keys[0], (), 0, period)
    left_slot = jax.random.randint(keys[1], (devices,), 0, width)
    right_slot = jax.random.randint(keys[2], (devices,), 0, width)
    coin = jax.random.randint(keys[3], (devices,), 0, 2)
    index = jnp.arange(devices, dtype=jnp.int32)
    is_left = (index - phase) % period < stride
    partner = jnp.where(is_left, (index + stride) % devices, (index - stride) % devices)
    leader = jnp.where(is_left, index, partner)
    mine = jnp.where(is_left, left_slot[leader], right_slot[leader])
    theirs = jnp.where(is_left, right_slot[leader], left_slot[leader])
    swapping = coin[leader] == 1
    incoming = table[partner, theirs]
    column = jnp.arange(width, dtype=jnp.int32)[None, :] == mine[:, None]
    return jnp.where(column & swapping[:, None], incoming[:, None], table)


def draw_new_slot(key, part):
    devices = SPANS // CH_DEV
    table = jnp.arange(SPANS, dtype=jnp.int32).reshape(devices, CH_DEV)
    table = swap_round(jax.random.fold_in(key, 11), table, 1, 2)
    table = swap_round(jax.random.fold_in(key, 12), table, 2, 4)
    return jnp.zeros((SPANS,), jnp.int32).at[table.reshape(-1)].set(jnp.arange(SPANS, dtype=jnp.int32))


def rough_noise(key, shape):
    return jax.random.truncated_normal(key, -6.0, 6.0, shape, jnp.float32)


def fixed_pattern():
    dims = jnp.arange(HEAD_DIM, dtype=jnp.int32)
    return jnp.where((dims * 37 + 11) % 8 < 4, 1.0, -1.0).astype(jnp.float32)


def self_plan(key):
    keys = jax.random.split(jax.random.fold_in(key, 71), 7)
    span_index = jnp.arange(SPANS, dtype=jnp.int32)[:, None]
    head_index = jnp.arange(HEADS, dtype=jnp.int32)[None, :]
    first_span = jax.random.randint(keys[0], (), 0, SPANS)
    first_head = jax.random.randint(keys[1], (), 0, HEADS)
    forced = (span_index == first_span) & (head_index == first_head)
    planted = (jax.random.randint(keys[2], (SPANS, HEADS), 0, 16) == 0) | forced
    signs = (2 * jax.random.randint(keys[3], (SPANS, HEADS, HEAD_DIM), 0, 2) - 1).astype(jnp.float32)
    query_steps = jnp.where(forced, 185, jax.random.randint(keys[4], (SPANS, HEADS), 112, 186))
    key_steps = jnp.where(forced, 185, jax.random.randint(keys[5], (SPANS, HEADS), 144, 186))
    own_first = jax.random.randint(keys[6], (SPANS, HEADS), 0, 2) == 1
    higher = key_steps.astype(jnp.float32) / 32.0
    lower = (key_steps - 2).astype(jnp.float32) / 32.0
    query_scale = query_steps.astype(jnp.float32) / 32.0
    own_scale = jnp.where(own_first, higher, lower)
    cached_scale = jnp.where(own_first, lower, higher)
    return (planted, signs, query_scale, own_scale, cached_scale)


def draw_token_qkv(key, part):
    base = rough_noise(jax.random.fold_in(key, 1), (3, SPANS, HEADS, HEAD_DIM))
    planted, signs, query_scale, own_scale, cached_scale = self_plan(key)
    mask = planted[:, :, None]
    query_part = jnp.where(mask, query_scale[:, :, None] * signs, base[0])
    key_part = jnp.where(mask, own_scale[:, :, None] * signs, base[1])
    stacked = jnp.stack([query_part, key_part, base[2]])
    return stacked.reshape(3, SPANS, D).astype(jnp.bfloat16)


def draw_self_cache(key, part):
    base = rough_noise(jax.random.fold_in(key, 2), (2, SPANS, SLOTS, HEADS, HEAD_DIM))
    planted, signs, query_scale, own_scale, cached_scale = self_plan(key)
    first_keys = jnp.where(planted[:, :, None], cached_scale[:, :, None] * signs, base[0, :, 0])
    base = base.at[0, :, 0].set(first_keys)
    return base.reshape(2, SPANS, SLOTS, D).astype(jnp.bfloat16)


def draw_cross_kv(key, part):
    base = rough_noise(jax.random.fold_in(key, 3), (2, SPANS, ENC, HEADS, HEAD_DIM))
    keys = jax.random.split(jax.random.fold_in(key, 73), 5)
    span_index = jnp.arange(SPANS, dtype=jnp.int32)
    forced_span = jax.random.randint(keys[0], (), 0, SPANS)
    planted = (jax.random.randint(keys[1], (SPANS,), 0, 8) == 0) | (span_index == forced_span)
    first_frame = jax.random.randint(keys[2], (SPANS,), 0, ENC)
    second_frame = (first_frame + 1 + jax.random.randint(keys[3], (SPANS,), 0, ENC - 1)) % ENC
    key_steps = jnp.where(span_index == forced_span, 184, jax.random.randint(keys[4], (SPANS,), 96, 186))
    higher = key_steps.astype(jnp.float32) / 32.0
    lower = (key_steps - 2).astype(jnp.float32) / 32.0
    frame = jnp.arange(ENC, dtype=jnp.int32)[None, :]
    at_first = frame == first_frame[:, None]
    at_second = frame == second_frame[:, None]
    scale = jnp.where(at_first, higher[:, None], jnp.where(at_second, lower[:, None], 0.0))
    use = planted[:, None] & (at_first | at_second)
    pattern = fixed_pattern()
    key_part = jnp.where(use[:, :, None, None], scale[:, :, None, None] * pattern[None, None, None, :], base[0])
    stacked = jnp.stack([key_part, base[1]])
    return stacked.reshape(2, SPANS, ENC, D).astype(jnp.bfloat16)


def bias_plan(key):
    keys = jax.random.split(jax.random.fold_in(key, 91), 3)
    bias = 0.5 * jax.random.truncated_normal(keys[0], -6.0, 6.0, (D,), jnp.float32)
    head_index = jnp.arange(HEADS, dtype=jnp.int32)
    chosen_head = jax.random.randint(keys[1], (), 0, HEADS)
    heads_on = (jax.random.randint(keys[2], (HEADS,), 0, 4) == 0) | (head_index == chosen_head)
    return (bias, heads_on)


def draw_ln_bias(key, part):
    bias, heads_on = bias_plan(key)
    return bias


def draw_query_proj(key, part):
    bias, heads_on = bias_plan(key)
    weight_key = jax.random.fold_in(key, 92)
    weight = jax.random.truncated_normal(weight_key, -6.0, 6.0, (D, D), jnp.float32) * D ** (-0.5)
    direction = 5.0 * jnp.where(heads_on[:, None], fixed_pattern()[None, :], 0.0).reshape(D)
    norm_sq = jnp.maximum(jnp.sum(bias * bias), D / 8.0)
    weight = weight + (bias / norm_sq)[:, None] * direction[None, :]
    return weight.astype(jnp.bfloat16)


def set_ends(drawn, own_key, low, high):
    extent = drawn.shape
    place = [jax.random.randint(jax.random.fold_in(own_key, axis), (), 0, extent[axis]) for axis in range(len(extent))]
    drawn = drawn.at[tuple(place)].set(low)
    longest = extent.index(max(extent))
    place[longest] = (place[longest] + 1) % extent[longest]
    return drawn.at[tuple(place)].set(high)


def shard_levels(key, shape, shards, low, top_value):
    factor_of, own = 1.0, jax.random.fold_in(key, 6)
    for dim, shards_of in shards:
        heights = jnp.exp(jax.random.uniform(jax.random.fold_in(own, dim), (shards_of,), jnp.float32, low / len(shards), top_value / len(shards)))
        factor_of = factor_of * jnp.repeat(heights, shape[dim] // shards_of).reshape([-1 if axis == dim else 1 for axis in range(len(shape))])
    return factor_of


def noise(key, extent, deviation, reach, shards=(), kind=jnp.bfloat16):
    values = deviation * jax.random.normal(key, extent, jnp.float32)
    if shards:
        values = values * shard_levels(key, extent, shards, -0.22, 0.18)
    return jnp.clip(values, -reach, reach).astype(kind)


def setup_inputs(seed: int = 0, part: int = 0) -> dict:
    seeds = jax.random.split(jax.random.key(seed), 12)
    part_splits = jax.random.split(jax.random.fold_in(seeds[11], part), 12)
    return {
        "hidden": noise(part_splits[0], (SPANS, D), 1.0, 6.0, ((0, 128),)),
        "token_qkv": draw_token_qkv(jax.random.fold_in(jax.random.fold_in(seeds[11], part), 71), part),
        "self_cache": draw_self_cache(jax.random.fold_in(jax.random.fold_in(seeds[11], part), 71), part),
        "cross_kv": draw_cross_kv(jax.random.fold_in(jax.random.fold_in(seeds[11], part), 71), part),
        "cache_len": set_ends(jax.random.randint(part_splits[4], (SPANS,), 1, SLOTS), jax.random.fold_in(part_splits[4], 1), 1, SLOTS - 1).astype(jnp.int32),
        "finished": set_ends((jax.random.randint(part_splits[5], (SPANS,), 0, 4) < 1).astype(jnp.int32), jax.random.fold_in(part_splits[5], 1), 0, 1),
        "new_slot": draw_new_slot(jax.random.fold_in(jax.random.fold_in(seeds[11], part), 71), part),
        "out_proj": noise(seeds[7], (D, D), D ** -0.5, 0.15625, ((0, 2),)),
        "ln_gain": jnp.clip(1.0 + 0.1 * jax.random.normal(seeds[8], (D,), jnp.float32), 0.5, 1.5),
        "ln_bias": draw_ln_bias(jax.random.fold_in(seeds[11], 71), part),
        "query_proj": draw_query_proj(jax.random.fold_in(seeds[11], 71), part),
    }


def reference(hidden, token_qkv, self_cache, cross_kv, cache_len, finished, new_slot, out_proj, ln_gain, ln_bias, query_proj):
    head_count = D // HEAD_DIM
    factor = HEAD_DIM ** (-0.5)
    new_query = token_qkv[0].astype(jnp.float32).reshape(SPANS, head_count, HEAD_DIM)
    new_key = token_qkv[1].astype(jnp.float32).reshape(SPANS, head_count, HEAD_DIM)
    new_value = token_qkv[2].astype(jnp.float32).reshape(SPANS, head_count, HEAD_DIM)
    cache_keys = self_cache[0].astype(jnp.float32).reshape(SPANS, SLOTS, head_count, HEAD_DIM)
    cache_values = self_cache[1].astype(jnp.float32).reshape(SPANS, SLOTS, head_count, HEAD_DIM)
    scores = jnp.einsum('chd,cthd->cht', new_query, cache_keys) * factor
    position = jnp.arange(SLOTS, dtype=jnp.int32)
    usable = position[None, None, :] < cache_len[:, None, None]
    scores = jnp.where(usable, scores, -1e+30)
    own_score = lax.optimization_barrier(jnp.sum(new_query * new_key, axis=-1)) * factor
    highest = jnp.maximum(lax.optimization_barrier(jnp.max(scores, axis=-1)), own_score)
    cache_weight = jnp.where(usable, jnp.exp(scores - highest[..., None]), 0.0)
    own_weight = jnp.exp(own_score - highest)
    total = lax.optimization_barrier(jnp.sum(cache_weight, axis=-1)) + own_weight
    cache_weight = (cache_weight / total[..., None]).astype(jnp.bfloat16)
    own_weight = (own_weight / total).astype(jnp.bfloat16)
    context = jnp.einsum('cht,cthd->chd', cache_weight.astype(jnp.float32), cache_values)
    context = context + own_weight.astype(jnp.float32)[..., None] * new_value
    context = context.astype(jnp.bfloat16).reshape(SPANS, D)
    resid = hidden.astype(jnp.float32) + jnp.dot(context, out_proj, preferred_element_type=jnp.float32)
    centre = lax.optimization_barrier(jnp.mean(resid, axis=-1, keepdims=True))
    spread = lax.optimization_barrier(jnp.mean((resid - centre) ** 2, axis=-1, keepdims=True))
    normed = ((resid - centre) * lax.rsqrt(spread + 1e-05) * ln_gain + ln_bias).astype(jnp.bfloat16)
    cross_query = jnp.dot(normed, query_proj, preferred_element_type=jnp.float32).astype(jnp.bfloat16)
    cross_query = cross_query.astype(jnp.float32).reshape(SPANS, head_count, HEAD_DIM)
    cross_keys = cross_kv[0].astype(jnp.float32).reshape(SPANS, ENC, head_count, HEAD_DIM)
    cross_values = cross_kv[1].astype(jnp.float32).reshape(SPANS, ENC, head_count, HEAD_DIM)
    cross_scores = jnp.einsum('chd,cthd->cht', cross_query, cross_keys) * factor
    cross_high = lax.optimization_barrier(jnp.max(cross_scores, axis=-1, keepdims=True))
    cross_exp = jnp.exp(cross_scores - cross_high)
    cross_weight = (cross_exp / lax.optimization_barrier(jnp.sum(cross_exp, axis=-1, keepdims=True))).astype(jnp.bfloat16)
    cross_context = jnp.einsum('cht,cthd->chd', cross_weight.astype(jnp.float32), cross_values).reshape(SPANS, D)
    alive = finished == 0
    decoded = jnp.where(alive[:, None], cross_context, 0.0).astype(jnp.bfloat16)
    slot_pos = position[None, :, None]
    length = cache_len[:, None, None]

    def extend(older, fresh):
        grown = jnp.where(slot_pos < length, older, jnp.where(slot_pos == length, fresh[:, None, :], jnp.zeros_like(older)))
        return jnp.where(alive[:, None, None], grown, jnp.zeros_like(older))
    updated = jnp.stack([extend(self_cache[0], token_qkv[1]), extend(self_cache[1], token_qkv[2])])
    moved_cache = jnp.zeros_like(self_cache).at[:, new_slot].set(updated)
    moved_out = jnp.zeros((SPANS, D), jnp.bfloat16).at[new_slot].set(decoded)
    return (moved_cache, moved_out)
```

```python
import functools

import jax
import jax.numpy as jnp
from jax import lax
from jax.experimental import pallas as pl
from jax.experimental.pallas import tpu as pltpu
from jax.sharding import PartitionSpec as P

HEAD_DIM = 64
REACH = 3
ROW = 4
HALVES = 2
MESH = pl.DeviceIdType.MESH
F32 = jnp.float32
BF16 = jnp.bfloat16


def spread_heads(row, rows):
    width = row.shape[-1]
    head = lax.broadcasted_iota(jnp.int32, (rows, width), 0)
    lane_head = lax.broadcasted_iota(jnp.int32, (rows, width), 1) // HEAD_DIM
    return jnp.where(head == lane_head, jnp.broadcast_to(row, (rows, width)), 0.0)


def gather_heads(product):
    rows, width = product.shape
    head = lax.broadcasted_iota(jnp.int32, (rows, width), 0)
    lane_head = lax.broadcasted_iota(jnp.int32, (rows, width), 1) // HEAD_DIM
    return jnp.sum(jnp.where(head == lane_head, product, 0.0), axis=0, keepdims=True)


def two_rows(first, second, rows):
    shape = (rows, first.shape[-1])
    at = lax.broadcasted_iota(jnp.int32, shape, 0)
    return jnp.where(at == 0, jnp.broadcast_to(first, shape), jnp.broadcast_to(second, shape))


def attend(query_row, keys, values, last):
    scores = lax.dot_general(
        spread_heads(query_row, 16).astype(BF16),
        keys,
        (((1,), (1,)), ((), ())),
        preferred_element_type=F32,
    ) * (HEAD_DIM**-0.5)
    if last is not None:
        usable = lax.broadcasted_iota(jnp.int32, scores.shape, 1) <= last
        scores = jnp.where(usable, scores, -1e30)
    weight = jnp.exp(scores - jnp.max(scores, axis=-1, keepdims=True))
    if last is not None:
        weight = jnp.where(usable, weight, 0.0)
    weight = (weight / jnp.sum(weight, axis=-1, keepdims=True)).astype(BF16)
    return gather_heads(jnp.dot(weight, values, preferred_element_type=F32))


def kernel(
    devices,
    hidden_h,
    qkv_h,
    cache_h,
    cross_h,
    len_h,
    fin_h,
    slot_h,
    wo_h,
    gain_h,
    bias_h,
    wq_h,
    moved_h,
    out_ref,
    hidden,
    qkv,
    cache,
    cross,
    lens,
    fins,
    slots,
    wo,
    gain,
    bias,
    wq,
    partial,
    arrived,
    info,
    rows_out,
    *rest,
):
    chunks = 2 * HALVES
    cands, stages = rest[:chunks], rest[chunks : 2 * chunks]
    (load_sem, own_sem, info_s, info_r, p1_s, p1_r, z_s, z_r, p3_s, p3_r, mp_s, mp_r, out_s, out_r) = rest[2 * chunks :]
    spans, positions = cache.shape[1], cache.shape[2]
    quarter = positions // ROW
    piece = quarter // HALVES
    me = lax.axis_index("batch")
    x = lax.rem(me, ROW)
    row_start = me - x
    core = lax.axis_index("mp")

    def device(dz, column):
        return {"batch": lax.rem(row_start + dz * ROW + devices, devices) + column}

    def column(dx):
        return lax.rem(x + dx + ROW, ROW)

    def remote(src, dst, send, recv, to):
        return pltpu.make_async_remote_copy(
            src_ref=src, dst_ref=dst, send_sem=send, recv_sem=recv, device_id=to, device_id_type=MESH
        )

    order = [
        (len_h, lens),
        (fin_h, fins),
        (slot_h, slots),
        (qkv_h, qkv),
        (cache_h.at[0], cache.at[0]),
        (cache_h.at[1], cache.at[1]),
        (wo_h, wo),
        (hidden_h, hidden),
        (gain_h, gain),
        (bias_h, bias),
        (wq_h, wq),
        (cross_h, cross),
    ]
    loads = [pltpu.make_async_copy(src, dst, load_sem.at[n]) for n, (src, dst) in enumerate(order)]
    for load in loads:
        load.start()

    barrier = pltpu.get_barrier_semaphore()
    peers = [(dz, dx) for dz in (0, -1, 1) for dx in range(ROW) if (dz, dx) != (0, 0)]
    for dz, dx in peers:
        pl.semaphore_signal(barrier, inc=1, device_id=device(dz, column(dx)), device_id_type=MESH)
    pl.semaphore_signal(barrier, inc=1, device_id={"mp": 1 - core}, device_id_type=MESH)

    for load in loads[:4]:
        load.wait()
    at = lax.broadcasted_iota(jnp.int32, (positions, cache.shape[3]), 0)
    for a in range(2):
        loads[4 + a].wait()
        for j in range(spans):
            older = cache[a, j].astype(F32)
            fresh = jnp.broadcast_to(qkv[1 + a, j : j + 1].astype(F32), older.shape)
            length = lens[j]
            grown = jnp.where(at < length, older, jnp.where(at == length, fresh, 0.0))
            alive = jnp.where(at < jnp.where(fins[j] == 0, positions, 0), grown, 0.0)
            cache[a, j] = alive.astype(BF16)
    for c in range(chunks):
        a, half = c // HALVES, c % HALVES
        start = pl.multiple_of(quarter * x + piece * half, piece)
        for j in range(spans):
            cands[c][spans * x + j] = cache[a, j, pl.ds(start, piece), :]
    lane = lax.broadcasted_iota(jnp.int32, (1, 128), 1)
    info[ROW + x] = jnp.where(lane == 0, slots[0], slots[1])

    pl.semaphore_wait(barrier, len(peers) + 1)

    info_copies = []
    for n, (dz, dx) in enumerate(peers):
        copy = remote(
            info.at[ROW + x], info.at[(1 - dz) * ROW + x], info_s.at[n], info_r.at[n], device(dz, column(dx))
        )
        copy.start()
        info_copies.append(copy)

    first = []
    for c in range(chunks):
        a, half = c // HALVES, c % HALVES
        for n, dx in enumerate((1, 3, 2)):
            to = column(dx)
            start = pl.multiple_of(quarter * to + piece * half, piece)
            copy = remote(
                cache.at[a, :, pl.ds(start, piece), :],
                cands[c].at[pl.ds(spans * x, spans)],
                p1_s.at[c, n],
                p1_r.at[c, n],
                device(0, to),
            )
            copy.start()
            first.append(copy)

    base_up, base_down = ROW * spans, ROW * spans + REACH * spans

    def up(c, n, b):
        return remote(
            cands[c].at[pl.ds(spans * b, spans)],
            cands[c].at[pl.ds(base_up + spans * (b - 1), spans)],
            z_s.at[c, 0, n],
            z_r.at[c, 0, b - 1],
            device(1, x),
        )

    def down(c, n, b):
        return remote(
            cands[c].at[pl.ds(spans * b, spans)],
            cands[c].at[pl.ds(base_down + spans * b, spans)],
            z_s.at[c, 1, n],
            z_r.at[c, 1, b],
            device(-1, x),
        )

    def pass_on(c, n, b):
        @pl.when(b >= 1)
        def _():
            up(c, n, b).start()

        @pl.when(b <= REACH - 1)
        def _():
            down(c, n, b).start()

    for c in range(chunks):
        pass_on(c, 0, x)

    def relay(c):
        for n, dx in enumerate((1, 3, 2)):
            first[c * 3 + n].wait_recv()
            pass_on(c, n + 1, column(-dx))

    contexts = []
    for j in range(spans):
        contexts.append(attend(qkv[0, j : j + 1].astype(F32), cache[0, j], cache[1, j], lens[j]))
    context = two_rows(contexts[0], contexts[1], 16).astype(BF16)
    loads[6].wait()
    partial[...] = jnp.dot(context, wo[...], preferred_element_type=F32)[:spans]
    swap = remote(partial, arrived, mp_s.at[0], mp_r.at[0], {"mp": 1 - core})
    swap.start()
    relay(0)
    for load in loads[7:]:
        load.wait()
    swap.wait()
    resid = hidden[...].astype(F32) + (partial[...] + arrived[...])
    centre = jnp.mean(resid, axis=-1, keepdims=True)
    spread = jnp.mean((resid - centre) ** 2, axis=-1, keepdims=True)
    normed = (resid - centre) * lax.rsqrt(spread + 1e-05) * gain[...] + bias[...]
    normed = two_rows(normed[0:1], normed[1:2], 16).astype(BF16)
    cross_query = jnp.dot(normed, wq[...], preferred_element_type=F32).astype(BF16).astype(F32)
    relay(1)
    decoded = []
    for j in range(spans):
        got = attend(cross_query[j : j + 1], cross[0, j], cross[1, j], None)
        decoded.append(jnp.where(lane[:, :1] < jnp.where(fins[j] == 0, 1, 0), got, 0.0))
    rows_out[REACH] = two_rows(decoded[0], decoded[1], spans).astype(BF16)
    out_copies = []
    for n, d in enumerate([d for d in range(-REACH, REACH + 1) if d != 0]):
        to = {"batch": lax.rem(me + d + devices, devices)}
        copy = remote(rows_out.at[REACH], rows_out.at[REACH - d], out_s.at[n], out_r.at[n], to)
        copy.start()
        out_copies.append(copy)
    relay(2)
    relay(3)

    for copy in info_copies:
        copy.wait_recv()
    table = info[...].reshape(3 * ROW, 128)
    source = lax.broadcasted_iota(jnp.int32, table.shape, 0)
    local = lax.broadcasted_iota(jnp.int32, table.shape, 1)
    source_x = source % ROW
    below, above = source < ROW, source >= 2 * ROW
    number = spans * source_x + local
    number = jnp.where(below, number + base_up - spans, jnp.where(above, number + base_down, number))
    counted = local < spans

    def look_up(slot, values, most):
        return jnp.minimum(jnp.max(jnp.where(counted & (table == slot), values, 0)), most)

    takes = [look_up(spans * row_start + n, number, cands[0].shape[0] - 1) for n in range(spans * ROW)]
    away = source - ROW - x + REACH
    mine = [
        (look_up(spans * me + n, away, 2 * REACH), look_up(spans * me + n, local, spans - 1))
        for n in range(spans)
    ]

    third = []
    owns = []
    for c in range(chunks):
        a, half = c // HALVES, c % HALVES
        for n in range(3):
            remote(cands[c].at[pl.ds(0, spans)], cands[c].at[pl.ds(base_up + spans * n, spans)], z_s.at[c, 0, n], z_r.at[c, 0, n], device(1, x)).wait_recv()
            remote(cands[c].at[pl.ds(0, spans)], cands[c].at[pl.ds(base_down + spans * n, spans)], z_s.at[c, 1, n], z_r.at[c, 1, n], device(-1, x)).wait_recv()
        for n in range(ROW):
            for l in range(spans):
                stages[c][n, l] = cands[c][takes[spans * n + l]]
        start = pl.multiple_of(quarter * x + piece * half, piece)
        where = moved_h.at[a, :, pl.ds(start, piece), :]
        for n, dx in enumerate((1, 3, 2)):
            to = column(dx)
            copy = remote(stages[c].at[to], where, p3_s.at[c, n], p3_r.at[c, n], device(0, to))
            copy.start()
            third.append(copy)
        own = pltpu.make_async_copy(stages[c].at[x], where, own_sem.at[c])
        own.start()
        owns.append(own)

    for copy in out_copies:
        copy.wait_recv()
    results = []
    for source_of, local_of in mine:
        both = rows_out[source_of].astype(F32)
        results.append(jnp.where(jnp.broadcast_to(local_of, both[:1].shape) == 0, both[0:1], both[1:2]))
    out_ref[...] = two_rows(results[0], results[1], spans).astype(BF16)

    for copy in third:
        copy.wait_recv()
    for own in owns:
        own.wait()
    for copy in info_copies + first + out_copies + third:
        copy.wait_send()
    for c in range(chunks):
        for n, dx in enumerate((0, 1, 3, 2)):
            b = column(-dx)

            @pl.when(b >= 1)
            def _():
                up(c, n, b).wait_send()

            @pl.when(b <= REACH - 1)
            def _():
                down(c, n, b).wait_send()


def body(
    hidden,
    token_qkv,
    self_cache,
    cross_kv,
    cache_len,
    finished,
    new_slot,
    out_proj,
    ln_gain,
    ln_bias,
    query_proj,
):
    spans, full_width = hidden.shape
    _, _, slots, width = self_cache.shape
    chunks = 2 * HALVES
    piece = slots // ROW // HALVES
    dma, vmem, smem = pltpu.SemaphoreType.DMA, pltpu.VMEM, pltpu.SMEM
    gain, bias = ln_gain.reshape(1, -1), ln_bias.reshape(1, -1)
    inputs = (hidden, token_qkv, self_cache, cross_kv, cache_len, finished, new_slot, out_proj, gain, bias, query_proj)
    peers = 3 * ROW - 1
    candidates = spans * (ROW + 2 * REACH)
    scratch = [
        vmem(hidden.shape, BF16),
        vmem(token_qkv.shape, BF16),
        vmem(self_cache.shape, BF16),
        vmem(cross_kv.shape, BF16),
        smem(cache_len.shape, jnp.int32),
        smem(finished.shape, jnp.int32),
        smem(new_slot.shape, jnp.int32),
        vmem(out_proj.shape, BF16),
        vmem(gain.shape, F32),
        vmem(bias.shape, F32),
        vmem(query_proj.shape, BF16),
        vmem((spans, full_width), F32),
        vmem((spans, full_width), F32),
        vmem((3 * ROW, 1, 128), jnp.int32),
        vmem((2 * REACH + 1, spans, width), BF16),
        *[vmem((candidates, piece, width), BF16) for _ in range(chunks)],
        *[vmem((ROW, spans, piece, width), BF16) for _ in range(chunks)],
        dma((len(inputs) + 1,)),
        dma((chunks,)),
        dma((peers,)),
        dma((peers,)),
        dma((chunks, 3)),
        dma((chunks, 3)),
        dma((chunks, 2, ROW)),
        dma((chunks, 2, 3)),
        dma((chunks, 3)),
        dma((chunks, 3)),
        dma((1,)),
        dma((1,)),
        dma((2 * REACH,)),
        dma((2 * REACH,)),
    ]
    return pl.pallas_call(
        functools.partial(kernel, lax.axis_size("batch")),
        out_shape=(
            jax.ShapeDtypeStruct(self_cache.shape, BF16),
            jax.ShapeDtypeStruct((spans, width), BF16),
        ),
        in_specs=[pl.BlockSpec(memory_space=pl.ANY)] * len(inputs),
        out_specs=(pl.BlockSpec(memory_space=pl.ANY), pl.BlockSpec(memory_space=vmem)),
        scratch_shapes=scratch,
        compiler_params=pltpu.CompilerParams(collective_id=0, has_side_effects=True),
    )(*inputs)


def solution(mesh):
    placed = (
        P(("groups", "batch"), None),
        P(None, ("groups", "batch"), "mp"),
        P(None, ("groups", "batch"), None, "mp"),
        P(None, ("groups", "batch"), None, "mp"),
        P(("groups", "batch")),
        P(("groups", "batch")),
        P(("groups", "batch")),
        P("mp", None),
        P(),
        P(),
        P(None, "mp"),
    )
    return jax.shard_map(
        body,
        mesh=mesh,
        in_specs=placed,
        out_specs=(P(None, ("groups", "batch"), None, "mp"), P(("groups", "batch"), "mp")),
        check_vma=False,
    )
```
